32 devices in a mesh: member: 8 (over y, x, core), tensor: 4 (over z).
Axes of the slice: x: 2, y: 2, z: 4, core: 2. Of those that a mesh axis runs over, the one named last changes fastest.
Arguments:
- prompt_acts: bfloat16 [128, 5120], P(None, 'member'), may hold values from -6 to 6
- gate_weight: bfloat16 [5120, 13824], P('member', 'tensor'), may hold values from -0.078125 to 0.078125
- up_weight: bfloat16 [5120, 13824], P('member', 'tensor'), may hold values from -0.078125 to 0.078125
- down_weight: bfloat16 [13824, 5120], P('tensor', 'member'), may hold values from -0.0546875 to 0.0546875
- d_table: bfloat16 [128, 3, 4, 5120], P('member'), may hold values from -6 to 6
- f_table: bfloat16 [128, 3, 4, 13824], P('member', None, None, 'tensor'), may hold values from -6 to 6
- seeds: int32 [64], P('member'), may hold values from 0 to 15
- fitness: float32 [64], P('member'), may hold values from -6 to 6
Outputs:
- outputs: bfloat16 [64, 128, 5120], P('member', None, 'tensor')
- delta_gate: bfloat16 [5120, 13824], P('member', 'tensor')
- delta_up: bfloat16 [5120, 13824], P('member', 'tensor')
- delta_down: bfloat16 [13824, 5120], P('tensor', 'member')
The draws below stay inside these ranges and needn't reach their ends.
Inputs may be any that keep to these rules, and one draw needn't show every extreme that they name: Member m uses row (m // 8) * 16 + seeds[m] of both tables, a row in its own group's block.
All inputs are finite; a program needn't handle non-finite values.
Results may differ from the reference program's by a relative error of at most 0.025.
Values may be sent and summed in bfloat16 or wider, within the bound.
No kernel may reach another device: no remote copies, remote signals or barrier semaphores. Data moves between devices by JAX's collectives and lax.ppermute only.
A program may use at most 192 MiB of HBM per device.

```python
import math
import jax
import jax.numpy as jnp
from jax import lax

D = 5120
FFW = 13824
RANK = 4
MEM_DEV = 8
PROMPT = 128
POP = 64
POOL_DEV = 16
POOL = 128
N_TENSOR = 4


def set_ends(array, own_key, smallest, high):
    longest = array.shape.index(max(array.shape))
    spots = []
    for shift in (0, 1):
        where = [jax.random.randint(jax.random.fold_in(own_key, axis), (), 0, length) for axis, length in enumerate(array.shape)]
        where[longest] = (where[longest] + shift) % array.shape[longest]
        spots.append(tuple(where))
    return array.at[spots[0]].set(smallest).at[spots[1]].set(high)


def level_of(stream_key, shape, pieces, smallest, largest):
    factor_of = 1.0
    for dim, shards_of in pieces:
        heights = jax.random.uniform(jax.random.fold_in(jax.random.fold_in(stream_key, 6), dim), (shards_of,), jnp.float32, smallest / len(pieces), largest / len(pieces))
        factor_of = factor_of * jnp.repeat(jnp.exp(heights), shape[dim] // shards_of).reshape((-1,) + (1,) * (len(shape) - 1 - dim))
    return factor_of


def gaussian(stream_key, dims, width, bound, pieces=(), kind=jnp.bfloat16):
    result = jax.random.normal(stream_key, dims, jnp.float32) * width
    if len(pieces) > 0:
        result = level_of(stream_key, dims, pieces, -0.22, 0.18) * result
    return jnp.clip(result, min=-bound, max=bound).astype(kind)


def setup_inputs(seed: int = 0) -> dict:
    streams_of = jax.random.split(jax.random.key(seed), 9)
    return {
        "prompt_acts": gaussian(streams_of[0], (PROMPT, D), 1.0, 6.0, ((1, 8),)),
        "gate_weight": gaussian(streams_of[1], (D, FFW), D ** -0.5, 0.078125, ((0, 8), (1, 4))),
        "up_weight": gaussian(streams_of[2], (D, FFW), D ** -0.5, 0.078125, ((0, 8), (1, 4))),
        "down_weight": gaussian(streams_of[3], (FFW, D), FFW ** -0.5, 0.0546875, ((0, 4), (1, 8))),
        "d_table": gaussian(streams_of[4], (POOL, 3, RANK, D), 1.0, 6.0, ((0, 8),)),
        "f_table": gaussian(streams_of[5], (POOL, 3, RANK, FFW), 1.0, 6.0, ((0, 8), (3, 4))),
        "seeds": set_ends(jax.random.randint(streams_of[6], (POP,), 0, POOL_DEV), jax.random.fold_in(streams_of[6], 1), 0, POOL_DEV - 1).astype(jnp.int32),
        "fitness": gaussian(streams_of[7], (POP,), 1.0, 6.0, ((0, 8),), jnp.float32),
    }


perturb_gain = 0.5

def reference(prompt_acts, gate_weight, up_weight, down_weight, d_table, f_table, seeds, fitness):
    members = jnp.arange(POP, dtype=jnp.int32)
    factor_rows = (members // MEM_DEV * POOL_DEV + seeds).astype(jnp.int32)
    down_factor_rows = jnp.take(d_table, factor_rows, axis=0)
    f_rows = jnp.take(f_table, factor_rows, axis=0)
    base_gate = jnp.dot(prompt_acts, gate_weight, preferred_element_type=jnp.float32).astype(jnp.bfloat16)
    base_up = jnp.dot(prompt_acts, up_weight, preferred_element_type=jnp.float32).astype(jnp.bfloat16)
    shard = FFW // N_TENSOR
    down_blocks = down_weight.reshape(N_TENSOR, shard, D).astype(jnp.float32)

    def member_out(pair):
        d_fac, f_fac = pair
        proj_gate = (jnp.dot(prompt_acts, d_fac[0].T, preferred_element_type=jnp.float32) / math.sqrt(D)).astype(jnp.bfloat16)
        proj_up = (jnp.dot(prompt_acts, d_fac[1].T, preferred_element_type=jnp.float32) / math.sqrt(D)).astype(jnp.bfloat16)
        gate = base_gate.astype(jnp.float32) + perturb_gain * jnp.dot(proj_gate, f_fac[0], preferred_element_type=jnp.float32)
        up = base_up.astype(jnp.float32) + perturb_gain * jnp.dot(proj_up, f_fac[1], preferred_element_type=jnp.float32)
        hidden_state = (jax.nn.silu(gate) * up).astype(jnp.bfloat16)
        blocks = hidden_state.reshape(PROMPT, N_TENSOR, shard).astype(jnp.float32)
        partial_value = jnp.einsum('ptf,tfd->tpd', blocks, down_blocks, precision=lax.Precision.HIGHEST)
        summed = lax.optimization_barrier(jnp.sum(partial_value.astype(jnp.bfloat16).astype(jnp.float32), axis=0))
        proj_down = (jnp.dot(hidden_state, f_fac[2].T, preferred_element_type=jnp.float32) / math.sqrt(FFW)).astype(jnp.bfloat16)
        down_noise_delta = perturb_gain * jnp.dot(proj_down, d_fac[2], preferred_element_type=jnp.float32)
        return (summed + down_noise_delta).astype(jnp.bfloat16)
    outputs = lax.map(member_out, (down_factor_rows, f_rows))
    mean = jnp.sum(fitness) / POP
    spread = jnp.sum((fitness - mean) ** 2) / POP
    score = (fitness - mean) / jnp.sqrt(spread + 1.0)
    weighted = (down_factor_rows.astype(jnp.float32) * score[:, None, None, None]).astype(jnp.bfloat16)
    scale = 1.0 / math.sqrt(POP * RANK)
    w_gate = weighted[:, 0].reshape(POP * RANK, D)
    w_up = weighted[:, 1].reshape(POP * RANK, D)
    w_down = weighted[:, 2].reshape(POP * RANK, D)
    f_gate = f_rows[:, 0].reshape(POP * RANK, FFW)
    f_up = f_rows[:, 1].reshape(POP * RANK, FFW)
    down_factor_columns = f_rows[:, 2].reshape(POP * RANK, FFW)
    delta_gate = (jnp.dot(w_gate.T, f_gate, preferred_element_type=jnp.float32) * scale).astype(jnp.bfloat16)
    delta_up = (jnp.dot(w_up.T, f_up, preferred_element_type=jnp.float32) * scale).astype(jnp.bfloat16)
    delta_down = (jnp.dot(down_factor_columns.T, w_down, preferred_element_type=jnp.float32) * scale).astype(jnp.bfloat16)
    return (outputs, delta_gate, delta_up, delta_down)
```

```python
import functools
import math

import jax
import jax.numpy as jnp
from jax import lax
from jax.experimental import pallas as pl
from jax.experimental.pallas import tpu as pltpu
from jax.sharding import PartitionSpec as P

perturb_gain = 0.5
CHUNKS = 4


def peer_of(own, shift, count):
    if count & (count - 1) == 0:
        return own ^ shift
    return (shift + count - own) % count


def home(pairs):
    return all(src == dst for src, dst in pairs)


def hidden_kernel(core_ref, base_ref, pg_ref, pu_ref, fac_ref, w_ref, out_ref, pd_ref, hid_ref, *, piece, copies):
    hidden_cols = w_ref.shape[0]
    rows4 = pg_ref.shape[2]
    prompt_len = base_ref.shape[1]

    def fill(step, carry):
        cols = pl.ds(pl.multiple_of(step * piece, piece), piece)
        fg = fac_ref[0, 0:rows4, cols]
        fu = fac_ref[0, rows4 : 2 * rows4, cols]
        bg = base_ref[0, :, cols].astype(jnp.float32)
        bu = base_ref[1, :, cols].astype(jnp.float32)
        for s in range(copies):
            rows = slice(s * prompt_len, (s + 1) * prompt_len)
            gate = bg + jnp.dot(pg_ref[0, rows, :], fg, preferred_element_type=jnp.float32)
            up = bu + jnp.dot(pu_ref[0, rows, :], fu, preferred_element_type=jnp.float32)
            half = 0.5 * gate
            hid_ref[rows, cols] = ((half + half * jnp.tanh(half)) * up).astype(jnp.bfloat16)
        return carry

    lax.fori_loop(0, hidden_cols // piece, fill, 0)
    out_ref[0] = jnp.dot(hid_ref[...], w_ref[...], preferred_element_type=jnp.float32).astype(jnp.bfloat16)
    pd_ref[0] = lax.dot_general(
        hid_ref[...],
        fac_ref[0, 2 * rows4 : 3 * rows4, :],
        (((1,), (1,)), ((), ())),
        preferred_element_type=jnp.float32,
    )


def partials(core, base, p_gate, p_up, factors, weights, chunk, chunk_rows, n_tensor, ratio):
    hidden_cols, out_cols = weights.shape
    prompt_len = base.shape[1]
    rows4 = p_gate.shape[2]
    piece = next((p for p in (384, 256, 128) if hidden_cols % p == 0), hidden_cols)
    group = lambda j, c: peer_of(c[1], j, n_tensor) * ratio + c[0]
    grid_spec = pltpu.PrefetchScalarGridSpec(
        num_scalar_prefetch=1,
        grid=(n_tensor,),
        in_specs=[
            pl.BlockSpec(base.shape, lambda j, c: (0, 0, 0)),
            pl.BlockSpec((1, chunk_rows, rows4), lambda j, c: (group(j, c), chunk, 0)),
            pl.BlockSpec((1, chunk_rows, rows4), lambda j, c: (group(j, c), chunk, 0)),
            pl.BlockSpec((1, 3 * rows4, hidden_cols), lambda j, c: (group(j, c), 0, 0)),
            pl.BlockSpec(weights.shape, lambda j, c: (0, 0)),
        ],
        out_specs=[
            pl.BlockSpec((1, chunk_rows, out_cols), lambda j, c: (j, 0, 0)),
            pl.BlockSpec((1, chunk_rows, rows4), lambda j, c: (j, 0, 0)),
        ],
        scratch_shapes=[pltpu.VMEM((chunk_rows, hidden_cols), jnp.bfloat16)],
    )
    flops = 2 * n_tensor * chunk_rows * hidden_cols * out_cols
    return pl.pallas_call(
        functools.partial(hidden_kernel, piece=piece, copies=chunk_rows // prompt_len),
        grid_spec=grid_spec,
        out_shape=[
            jax.ShapeDtypeStruct((n_tensor, chunk_rows, out_cols), jnp.bfloat16),
            jax.ShapeDtypeStruct((n_tensor, chunk_rows, rows4), jnp.float32),
        ],
        compiler_params=pltpu.CompilerParams(vmem_limit_bytes=56 * 1024 * 1024),
        cost_estimate=pl.CostEstimate(
            flops=2 * flops, bytes_accessed=2 * hidden_cols * out_cols, transcendentals=n_tensor * chunk_rows * hidden_cols
        ),
    )(core, base, p_gate, p_up, factors, weights)


def shards(
    prompt_acts, gate_weight, up_weight, down_weight, d_table, f_table, seeds, fitness, n_member, n_tensor
):
    members = seeds.shape[0]
    prompt_len = prompt_acts.shape[0]
    rank_size = d_table.shape[2]
    width = d_table.shape[3]
    width_cols = prompt_acts.shape[1]
    hidden_cols = gate_weight.shape[1]
    ffw = hidden_cols * n_tensor
    rows4 = members * rank_size
    ratio = n_member // n_tensor
    population = members * n_member
    my_member = lax.axis_index("member")
    my_tensor = lax.axis_index("tensor")
    core = my_member % ratio

    f_sel = jnp.take(f_table, seeds, axis=0, mode="clip")
    f_rows = f_sel.transpose(1, 0, 2, 3).reshape(3 * rows4, hidden_cols)
    f_all = lax.all_gather(f_rows, "member", axis=0, tiled=False)

    d_sel = jnp.take(d_table, seeds, axis=0, mode="clip")
    d_rows = d_sel.transpose(1, 0, 2, 3).reshape(3 * rows4, width)
    fit_hi = fitness.astype(jnp.bfloat16)
    fit_lo = (fitness - fit_hi.astype(jnp.float32)).astype(jnp.bfloat16)
    fit_rows = jnp.pad(jnp.stack([fit_hi, fit_lo]), ((0, 14), (0, width_cols - members)))
    d_send = jnp.stack(
        [
            jnp.concatenate([d_rows[:, k * width_cols : (k + 1) * width_cols], fit_rows], axis=0)
            for k in range(n_member)
        ]
    )
    d_recv = lax.all_to_all(d_send, "member", split_axis=0, concat_axis=0, tiled=True)

    gate_part = jnp.dot(prompt_acts, gate_weight, preferred_element_type=jnp.float32).astype(jnp.bfloat16)
    up_part = jnp.dot(prompt_acts, up_weight, preferred_element_type=jnp.float32).astype(jnp.bfloat16)
    in_rows = d_recv[:, : 2 * rows4].reshape(n_member * 2 * rows4, width_cols)
    proj_part = lax.dot_general(
        prompt_acts, in_rows, (((1,), (1,)), ((), ())), preferred_element_type=jnp.float32
    ).astype(jnp.bfloat16)
    sums_part = jnp.concatenate([gate_part, up_part, proj_part], axis=1)
    sum_cols = sums_part.shape[1]
    row_share = prompt_len // n_member
    sums_recv = lax.all_to_all(
        sums_part.reshape(n_member, row_share, sum_cols), "member", split_axis=0, concat_axis=0, tiled=True
    )
    col_scale = jnp.where(jnp.arange(sum_cols) < 2 * hidden_cols, 1.0, 1.0 / math.sqrt(width))
    sums_mine = (jnp.sum(sums_recv.astype(jnp.float32), axis=0) * col_scale).astype(jnp.bfloat16)
    sums = lax.all_gather(sums_mine, "member", axis=0, tiled=True)
    base = jnp.stack([sums[:, :hidden_cols], sums[:, hidden_cols : 2 * hidden_cols]])
    proj = sums[:, 2 * hidden_cols :].reshape(prompt_len, n_member, 2, rows4).transpose(2, 1, 0, 3)
    own_rows = (jnp.arange(rows4) // rank_size)[None, :] == jnp.arange(members)[:, None]
    masked = jnp.where(own_rows[None, None, :, None, :], perturb_gain * proj[:, :, None], 0.0).astype(jnp.bfloat16)
    masked = masked.reshape(2, n_member, members * prompt_len, rows4)

    if ratio == 1:
        weights = down_weight
    elif ratio == 2:
        other = lax.ppermute(down_weight, "member", [(g, g ^ 1) for g in range(n_member)])
        first = core == 0
        weights = jnp.concatenate(
            [jnp.where(first, down_weight, other), jnp.where(first, other, down_weight)], axis=1
        )
    else:
        weights = lax.all_gather(
            down_weight,
            "member",
            axis=1,
            tiled=True,
            axis_index_groups=[list(range(i, i + ratio)) for i in range(0, n_member, ratio)],
        )
    chunk_rows = members // CHUNKS * prompt_len
    own = my_member // ratio
    core_arg = jnp.stack([core, own]).astype(jnp.int32)
    swaps = [
        [(g, peer_of(g // ratio, shift, n_tensor) * ratio + g % ratio) for g in range(n_member)]
        for shift in range(n_tensor)
    ]
    own_slot = peer_of(own, own, n_tensor)
    summed, proj_here = [], []
    for chunk in range(CHUNKS):
        part, pd = partials(
            core_arg, base, masked[0], masked[1], f_all, weights, chunk, chunk_rows, n_tensor, ratio
        )
        proj_here.append(lax.dynamic_index_in_dim(pd, own_slot, 0, keepdims=False))
        moved = jnp.stack([
                part[shift] if home(swaps[shift]) else lax.ppermute(part[shift], "member", swaps[shift])
                for shift in range(n_tensor)
            ])
        ordered = [
            lax.dynamic_index_in_dim(moved, peer_of(own, chip, n_tensor), 0, keepdims=False)
            for chip in range(n_tensor)
        ]
        flat = jnp.concatenate(ordered, axis=0)
        summed.append(lax.psum_scatter(flat, "tensor", scatter_dimension=0, tiled=True))
    pd_all = jnp.concatenate(proj_here, axis=0).reshape(members, prompt_len, members, rank_size)
    pick = jnp.arange(members)[:, None] == jnp.arange(members)[None, :]
    pd_own = jnp.sum(jnp.where(pick[:, None, :, None], pd_all, 0.0), axis=2)
    proj_down = (lax.psum(pd_own, "tensor") / math.sqrt(ffw)).astype(jnp.bfloat16)
    out_cols = summed[0].shape[1]
    out_factor = lax.dynamic_slice_in_dim(d_sel[:, 2], my_tensor * out_cols, out_cols, 2)
    noise = perturb_gain * jnp.einsum("mpr,mrd->mpd", proj_down, out_factor, preferred_element_type=jnp.float32)
    total = jnp.concatenate(summed, axis=0).reshape(members, prompt_len, out_cols).astype(jnp.float32)
    outputs = (total + noise).astype(jnp.bfloat16)

    fit_recv = d_recv[:, 3 * rows4 : 3 * rows4 + 2, :members].astype(jnp.float32)
    fit_all = (fit_recv[:, 0] + fit_recv[:, 1]).reshape(population)
    mean = jnp.sum(fit_all) / population
    spread = jnp.sum((fit_all - mean) ** 2) / population
    score = (fit_all - mean) / jnp.sqrt(spread + 1.0)
    scale = 1.0 / math.sqrt(population * rank_size)
    row_score = jnp.repeat(score, rank_size).reshape(n_member, rows4, 1)
    ranks = population * rank_size
    d_part = lambda k: (d_recv[:, k * rows4 : (k + 1) * rows4].astype(jnp.float32) * row_score).astype(
        jnp.bfloat16
    ).reshape(ranks, width_cols)
    f_part = lambda k: f_all[:, k * rows4 : (k + 1) * rows4].reshape(ranks, hidden_cols)
    outer = lambda a, b: (
        lax.dot_general(a, b, (((0,), (0,)), ((), ())), preferred_element_type=jnp.float32) * scale
    ).astype(jnp.bfloat16)
    return (
        outputs,
        outer(d_part(0), f_part(0)),
        outer(d_part(1), f_part(1)),
        outer(f_part(2), d_part(2)),
    )


def solution(mesh):
    in_specs = (
        P(None, "member"),
        P("member", "tensor"),
        P("member", "tensor"),
        P("tensor", "member"),
        P("member", None, None, None),
        P("member", None, None, "tensor"),
        P("member"),
        P("member"),
    )
    out_specs = (
        P("member", None, "tensor"),
        P("member", "tensor"),
        P("member", "tensor"),
        P("tensor", "member"),
    )
    body = functools.partial(shards, n_member=mesh.shape["member"], n_tensor=mesh.shape["tensor"])
    return jax.shard_map(body, mesh=mesh, in_specs=in_specs, out_specs=out_specs, check_vma=False)
```
